32 devices in a mesh: node: 4 (over x, core), local: 8 (over z, y).
Axes of the slice: x: 2, y: 2, z: 4, core: 2. Of those that a mesh axis runs over, the one named last changes fastest.
Arguments:
- tokens: bfloat16 [2048, 7168], P(('node', 'local')), may hold values from -6 to 6
- routes: int32 [2048, 2], P(('node', 'local')), may hold values from 0 to 7, as said below
- scores: float32 [2048, 2], P(('node', 'local')), may hold values from 0.1 to 1
- gate_proj: bfloat16 [32, 7168, 512], P(('node', 'local')), may hold values from -0.0625 to 0.0625
- up_proj: bfloat16 [32, 7168, 512], P(('node', 'local')), may hold values from -0.0625 to 0.0625
- down_proj: bfloat16 [32, 512, 7168], P(('node', 'local')), may hold values from -0.125 to 0.125
Outputs:
- combined: bfloat16 [2048, 7168], P(('node', 'local'))
The draws below stay inside these ranges and needn't reach their ends.
Inputs may be any that keep to these rules, and one draw needn't show every extreme that they name: `routes`: each row names 2 different experts. The rows of one device name each expert at most 20 times, and in every draw one expert is named by exactly 20 rows of every device.
All inputs are finite; a program needn't handle non-finite values.
Results may differ from the reference program's by a relative error of at most 0.0085.
Values may be sent and summed in bfloat16 or wider, within the bound.
A program may use at most 192 MiB of HBM per device.

```python
import math
import jax
import jax.numpy as jnp
from jax import lax

D = 7168
FF = 2048
SHARDS = 4
TOP = 2
TOK_DEV = 64
FF_DEV = 512
EXPERTS = 8
MOST = 20
TOKENS = 2048


def draw_routes(key, part):
    blocks = TOKENS // TOK_DEV
    base_key = jax.random.fold_in(key, 11)
    key_hot, key_cycle, key_perm, key_order = jax.random.split(base_key, 4)
    hot_expert = jax.random.randint(key_hot, (), 0, EXPERTS)
    cycle_least = max(TOP, (TOK_DEV * TOP - MOST + MOST - 1) // MOST)
    cycle_length = jax.random.randint(key_cycle, (blocks,), cycle_least, EXPERTS)
    shuffles = jax.vmap(lambda one_key: jax.random.permutation(one_key, EXPERTS - 1))(jax.random.split(key_perm, blocks))
    others = shuffles + (shuffles >= hot_expert).astype(shuffles.dtype)
    token_ids = jnp.arange(TOK_DEV)[:, None]
    slot_ids = jnp.arange(TOP)[None, :]
    leading = token_ids < MOST
    other_pos = jnp.where(leading, token_ids * (TOP - 1) + slot_ids - 1, MOST * (TOP - 1) + (token_ids - MOST) * TOP + slot_ids)
    cycle_pos = jnp.mod(other_pos[None, :, :], cycle_length[:, None, None])
    chosen = jnp.take_along_axis(others, cycle_pos.reshape(blocks, -1), axis=1).reshape(blocks, TOK_DEV, TOP)
    chosen = jnp.where((leading & (slot_ids == 0))[None, :, :], hot_expert, chosen)
    token_order = jax.vmap(lambda one_key: jax.random.permutation(one_key, TOK_DEV))(jax.random.split(key_order, blocks))
    chosen = jnp.take_along_axis(chosen, token_order[:, :, None], axis=1)
    return chosen.reshape(TOKENS, TOP).astype(jnp.int32)


def shard_levels(stream_key, shape, shards, low, largest):
    factor_of, own = 1.0, jax.random.fold_in(stream_key, 6)
    for position, shards_of in shards:
        draws = jnp.exp(jax.random.uniform(jax.random.fold_in(own, position), (shards_of,), jnp.float32, low / len(shards), largest / len(shards)))
        factor_of = factor_of * jnp.repeat(draws, shape[position] // shards_of).reshape([-1 if axis == position else 1 for axis in range(len(shape))])
    return factor_of


def noise(stream_key, dims, spread, bound, pieces=(), kind=jnp.bfloat16):
    level = shard_levels(stream_key, dims, pieces, -0.22, 0.18) if pieces else 1.0
    entries = jax.random.normal(stream_key, dims, jnp.float32) * spread * level
    return jnp.minimum(jnp.maximum(entries, -bound), bound).astype(kind)


def setup_inputs(seed: int = 0) -> dict:
    splits = jax.random.split(jax.random.key(seed), 7)
    return {
        "tokens": noise(splits[0], (TOKENS, D), 1.0, 6.0, ((0, 32),)),
        "routes": draw_routes(jax.random.fold_in(splits[6], 71), 0),
        "scores": jnp.clip(jnp.exp(math.log(1.0) - 2.3025851 * jax.random.uniform(splits[2], (TOKENS, TOP), jnp.float32) ** shard_levels(splits[2], (TOKENS, TOP), ((0, 32),), -0.2, 0.2)), 0.1, 1.0),
        "gate_proj": noise(splits[3], (EXPERTS * SHARDS, D, FF_DEV), D ** -0.5, 0.0625, ((0, 32),)),
        "up_proj": noise(splits[4], (EXPERTS * SHARDS, D, FF_DEV), D ** -0.5, 0.0625, ((0, 32),)),
        "down_proj": noise(splits[5], (EXPERTS * SHARDS, FF_DEV, D), FF ** -0.5, 0.125, ((0, 32),)),
    }


SCALE = 2.827


def reference(tokens, routes, scores, gate_proj, up_proj, down_proj):
    pair_count = TOKENS * TOP
    weights = (SCALE * scores / jnp.sum(scores, axis=1, keepdims=True)).astype(jnp.bfloat16)
    flat_exp = routes.reshape(-1).astype(jnp.int32)
    sort_order = jnp.argsort(flat_exp, stable=True).astype(jnp.int32)
    labels = jnp.arange(EXPERTS, dtype=jnp.int32)
    counts = jnp.sum((flat_exp[:, None] == labels[None, :]).astype(jnp.int32), axis=0).astype(jnp.int32)
    padded = (((counts + 127) // 128) * 128).astype(jnp.int32)
    group_ends = jnp.cumsum(padded).astype(jnp.int32)
    group_starts = (group_ends - padded).astype(jnp.int32)
    sorted_starts = (jnp.cumsum(counts) - counts).astype(jnp.int32)
    sorted_exp = flat_exp[sort_order]
    rank_list = jnp.arange(pair_count, dtype=jnp.int32)
    target_pos = (group_starts[sorted_exp] + rank_list - sorted_starts[sorted_exp]).astype(jnp.int32)
    block_count = (pair_count + 127) // 128 + EXPERTS
    slot_table = jnp.full((block_count * 128,), pair_count, jnp.int32).at[target_pos].set(sort_order)
    block_first = jnp.arange(block_count, dtype=jnp.int32) * 128
    block_exp = jnp.minimum(jnp.sum((group_ends[None, :] <= block_first[:, None]).astype(jnp.int32), axis=1), EXPERTS - 1).astype(jnp.int32)
    pair_weight = jnp.concatenate([weights.reshape(-1).astype(jnp.float32), jnp.zeros((1,), jnp.float32)])
    padded_x = jnp.concatenate([tokens, jnp.zeros((1, D), jnp.bfloat16)], axis=0)

    def accumulate(running, block_num):
        row_index = lax.dynamic_slice_in_dim(slot_table, (block_num * 128).astype(jnp.int32), 128)
        token_index = (row_index // TOP).astype(jnp.int32)
        expert = block_exp[block_num]
        row_data = padded_x[token_index]
        row_weight = pair_weight[row_index]
        first_row = (expert * SHARDS).astype(jnp.int32)
        w_gate = lax.dynamic_slice_in_dim(gate_proj, first_row, SHARDS, 0).transpose(1, 0, 2).reshape(D, FF)
        w_up = lax.dynamic_slice_in_dim(up_proj, first_row, SHARDS, 0).transpose(1, 0, 2).reshape(D, FF)
        gate_act = jnp.dot(row_data, w_gate, preferred_element_type=jnp.float32)
        up_act = jnp.dot(row_data, w_up, preferred_element_type=jnp.float32)
        hidden = (jax.nn.silu(gate_act) * up_act).astype(jnp.bfloat16)
        w_down = lax.dynamic_slice_in_dim(down_proj, first_row, SHARDS, 0)
        summed = jnp.zeros((128, D), jnp.float32)
        for shard_num in range(SHARDS):
            partial_value = jnp.dot(hidden[:, shard_num * FF_DEV:(shard_num + 1) * FF_DEV], w_down[shard_num], preferred_element_type=jnp.float32).astype(jnp.bfloat16)
            summed = summed + partial_value.astype(jnp.float32)
        running = running.at[token_index].add(summed * row_weight[:, None])
        return running, None

    running = lax.scan(accumulate, jnp.zeros((TOKENS + 1, D), jnp.float32), jnp.arange(block_count, dtype=jnp.int32))[0]
    return running[:TOKENS].astype(jnp.bfloat16)
```

```python
import functools

import jax
import jax.numpy as jnp
from jax import lax
from jax.experimental import pallas as pl
from jax.experimental.pallas import tpu as pltpu
from jax.sharding import PartitionSpec as P

SHARDS = 4
SCALE = 2.827
MESH = pl.DeviceIdType.MESH


def place(groups):
    node = lax.axis_index("node")
    local = lax.axis_index("local")
    mine = node * groups + local // SHARDS
    block = local % SHARDS
    near = block + 1 - 2 * (block % 2)
    far = (block + 2) % SHARDS
    corner = (near + 2) % SHARDS

    def device(expert, which):
        return (expert // groups, (expert % groups) * SHARDS + which)

    return mine, block, near, far, corner, device


def greet(mine, block, near, far, device, experts):
    barrier = pltpu.get_barrier_semaphore()
    targets = [device((mine + r) % experts, block) for r in range(1, experts)]
    targets += [device(mine, near), device(mine, far)]
    for target in targets:
        pl.semaphore_signal(barrier, inc=1, device_id=target, device_id_type=MESH)
    pl.semaphore_wait(barrier, len(targets))


def over_far(r):
    return r % 4 == 0


def dispatch_kernel(experts, groups, bucket, out, own_sem, a_send, a_recv, b_send, b_recv, c_send, c_recv):
    mine, block, near, far, corner, device = place(groups)
    greet(mine, block, near, far, device, experts)

    def remote(src, dst, send, recv, target):
        return pltpu.make_async_remote_copy(
            src_ref=src, dst_ref=dst, send_sem=send, recv_sem=recv, device_id=target, device_id_type=MESH
        )

    spread = {}
    for r in range(1, experts):
        peer = (mine + r) % experts
        spread[r] = remote(bucket.at[peer], out.at[block, mine], a_send.at[r], a_recv.at[r], device(peer, block))
        spread[r].start()
    own = pltpu.make_async_copy(bucket.at[mine], out.at[block, mine], own_sem)
    own.start()

    order = list(range(experts))
    to_near, to_far, relay = {}, {}, {}

    def forward(r):
        source = (mine + experts - r) % experts
        if over_far(r):
            to_near[r].wait_recv()
            relay[r] = remote(out.at[near, source], out.at[near, source], c_send.at[r], c_recv.at[r], device(mine, far))
        else:
            to_far[r].wait_recv()
            relay[r] = remote(out.at[far, source], out.at[far, source], c_send.at[r], c_recv.at[r], device(mine, near))
        relay[r].start()

    for step, r in enumerate(order):
        source = (mine + experts - r) % experts
        if r == 0:
            src = bucket.at[mine]
        else:
            spread[r].wait_recv()
            src = out.at[block, source]
        to_near[r] = remote(src, out.at[block, source], b_send.at[0, r], b_recv.at[0, r], device(mine, near))
        to_far[r] = remote(src, out.at[block, source], b_send.at[1, r], b_recv.at[1, r], device(mine, far))
        to_near[r].start()
        to_far[r].start()
        if step >= 2:
            forward(order[step - 2])
    for r in order[-2:]:
        forward(r)
    for r in order:
        if over_far(r):
            to_far[r].wait_recv()
        else:
            to_near[r].wait_recv()
        relay[r].wait_recv()
    for r in order:
        if r:
            spread[r].wait_send()
        to_near[r].wait_send()
        to_far[r].wait_send()
        relay[r].wait_send()
    own.wait()


def combine_kernel(experts, groups, part, ret, held, total, back, a_send, a_recv, b_send, b_recv, c_send, c_recv):
    mine, block, near, far, corner, device = place(groups)
    greet(mine, block, near, far, device, experts)

    def remote(src, dst, send, recv, target):
        return pltpu.make_async_remote_copy(
            src_ref=src, dst_ref=dst, send_sem=send, recv_sem=recv, device_id=target, device_id_type=MESH
        )

    def wide(ref):
        return ref[...].astype(jnp.float32)

    order = list(range(1, experts)) + [0]
    relay, to_near, to_far, home = {}, {}, {}, {}
    for r in order:
        source = (mine + experts - r) % experts
        target = far if over_far(r) else near
        relay[r] = remote(part.at[corner, source], held.at[2, r], c_send.at[r], c_recv.at[r], device(mine, target))
        relay[r].start()
        if over_far(r):
            to_far[r] = remote(part.at[far, source], held.at[1, r], b_send.at[1, r], b_recv.at[1, r], device(mine, far))
            to_far[r].start()
        else:
            to_near[r] = remote(part.at[near, source], held.at[0, r], b_send.at[0, r], b_recv.at[0, r], device(mine, near))
            to_near[r].start()

    def send_home(r):
        source = (mine + experts - r) % experts
        to_near[r].wait_recv()
        to_far[r].wait_recv()
        value = (wide(part.at[block, source]) + wide(held.at[0, r]) + wide(held.at[1, r])).astype(jnp.bfloat16)
        if r == 0:
            ret[mine] = value
        else:
            back[r] = value
            home[r] = remote(back.at[r], ret.at[mine], a_send.at[r], a_recv.at[r], device(source, block))
            home[r].start()

    for step, r in enumerate(order):
        source = (mine + experts - r) % experts
        relay[r].wait_recv()
        if over_far(r):
            total[r] = (wide(part.at[near, source]) + wide(held.at[2, r])).astype(jnp.bfloat16)
            to_near[r] = remote(total.at[r], held.at[0, r], b_send.at[0, r], b_recv.at[0, r], device(mine, near))
            to_near[r].start()
        else:
            total[r] = (wide(part.at[far, source]) + wide(held.at[2, r])).astype(jnp.bfloat16)
            to_far[r] = remote(total.at[r], held.at[1, r], b_send.at[1, r], b_recv.at[1, r], device(mine, far))
            to_far[r].start()
        if step >= 2:
            send_home(order[step - 2])
    for r in order[-2:]:
        send_home(r)
    for r in order:
        if r:
            home[r].wait()
        relay[r].wait_send()
        to_near[r].wait_send()
        to_far[r].wait_send()


def sems(experts):
    dma = pltpu.SemaphoreType.DMA
    return [dma((experts,)), dma((experts,)), dma((2, experts)), dma((2, experts)), dma((experts,)), dma((experts,))]


def dispatch(bucket, groups):
    experts, cap, width = bucket.shape
    return pl.pallas_call(
        functools.partial(dispatch_kernel, experts, groups),
        out_shape=jax.ShapeDtypeStruct((SHARDS, experts, cap, width), bucket.dtype),
        in_specs=[pl.BlockSpec(memory_space=pltpu.VMEM)],
        out_specs=pl.BlockSpec(memory_space=pl.ANY),
        scratch_shapes=[pltpu.SemaphoreType.DMA] + sems(experts),
        compiler_params=pltpu.CompilerParams(collective_id=0, has_side_effects=True),
        name="dispatch",
    )(bucket)


def combine(part, groups):
    shards, experts, cap, width = part.shape
    block = (experts, cap, width)
    return pl.pallas_call(
        functools.partial(combine_kernel, experts, groups),
        out_shape=jax.ShapeDtypeStruct(block, part.dtype),
        in_specs=[pl.BlockSpec(memory_space=pltpu.VMEM)],
        out_specs=pl.BlockSpec(memory_space=pltpu.VMEM),
        scratch_shapes=[
            pltpu.VMEM((3,) + block, part.dtype),
            pltpu.VMEM(block, part.dtype),
            pltpu.VMEM(block, part.dtype),
        ]
        + sems(experts),
        compiler_params=pltpu.CompilerParams(
            collective_id=1, has_side_effects=True, vmem_limit_bytes=60 * 2**20
        ),
        name="combine",
    )(part)


def expert_block(rows, w_gate, w_up, w_down):
    gate_act = jnp.dot(rows, w_gate, preferred_element_type=jnp.float32)
    up_act = jnp.dot(rows, w_up, preferred_element_type=jnp.float32)
    hidden = (jax.nn.silu(gate_act) * up_act).astype(jnp.bfloat16)
    return jnp.dot(hidden, w_down, preferred_element_type=jnp.float32).astype(jnp.bfloat16)


def per_device(tokens, routes, scores, gate_proj, up_proj, down_proj):
    node_count = lax.axis_size("node")
    local_count = lax.axis_size("local")
    token_count, model_width = tokens.shape
    top_count = routes.shape[1]
    groups = local_count // SHARDS
    experts = node_count * groups
    per_expert = max(
        2, token_count * top_count // experts + token_count * top_count // (4 * experts)
    )
    cap = (per_expert + 7) // 8 * 8
    weights = (SCALE * scores / jnp.sum(scores, axis=1, keepdims=True)).astype(jnp.bfloat16)
    labels = jnp.arange(experts, dtype=jnp.int32)
    matches = routes[:, :, None] == labels[None, None, :]
    routed = jnp.any(matches, axis=1)
    dense_weight = jnp.sum(jnp.where(matches, weights.astype(jnp.float32)[:, :, None], 0.0), axis=1)
    position = jnp.cumsum(routed.astype(jnp.int32), axis=0) - 1
    slot_ids = jnp.arange(cap, dtype=jnp.int32)
    pick = routed.T[:, None, :] & (position.T[:, None, :] == slot_ids[None, :, None])
    slot_pick = pick.astype(jnp.bfloat16).reshape(experts * cap, token_count)
    slot_weight = jnp.where(pick, dense_weight.T[:, None, :], 0.0).astype(jnp.bfloat16)
    slot_weight = slot_weight.reshape(experts * cap, token_count)
    bucket = jnp.dot(slot_pick, tokens, preferred_element_type=jnp.float32).astype(jnp.bfloat16)
    gathered = dispatch(bucket.reshape(experts, cap, model_width), groups)
    rows = gathered.reshape(SHARDS * experts * cap, model_width)
    part = expert_block(rows, gate_proj[0], up_proj[0], down_proj[0])
    returned = combine(part.reshape(SHARDS, experts, cap, model_width), groups)
    combined = lax.dot_general(
        slot_weight,
        returned.reshape(experts * cap, model_width),
        (((0,), (0,)), ((), ())),
        preferred_element_type=jnp.float32,
    )
    return combined.astype(jnp.bfloat16)


def solution(mesh):
    return jax.shard_map(
        per_device,
        mesh=mesh,
        in_specs=(
            P(("node", "local"), None),
            P(("node", "local"), None),
            P(("node", "local"), None),
            P(("node", "local"), None, None),
            P(("node", "local"), None, None),
            P(("node", "local"), None, None),
        ),
        out_specs=P(("node", "local"), None),
        check_vma=False,
    )
```

```python
import functools

import jax
import jax.numpy as jnp
from jax import lax
from jax.experimental import pallas as pl
from jax.experimental.pallas import tpu as pltpu
from jax.sharding import PartitionSpec as P

SHARDS = 4
SCALE = 2.827
FOLD = 4
MESH = pl.DeviceIdType.MESH


def place(groups):
    node = lax.axis_index("node")
    local = lax.axis_index("local")
    mine = node * groups + local // SHARDS
    block = local % SHARDS
    near = block + 1 - 2 * (block % 2)
    far = (block + 2) % SHARDS
    corner = (near + 2) % SHARDS

    def device(expert, which):
        return (expert // groups, (expert % groups) * SHARDS + which)

    return mine, block, near, far, corner, device


def greet(mine, block, near, far, device, experts):
    barrier = pltpu.get_barrier_semaphore()
    targets = [device((mine + r) % experts, block) for r in range(1, experts)]
    targets += [device(mine, near), device(mine, far)]
    for target in targets:
        pl.semaphore_signal(barrier, inc=1, device_id=target, device_id_type=MESH)
    pl.semaphore_wait(barrier, len(targets))


def over_far(r):
    return r % 4 == 0


def rounds(experts, groups):
    same = [r for r in range(experts) if r % groups == 0]
    return same + [r for r in range(experts) if r % groups]


AHEAD = 4
LAG = 2


class Transfer:
    def __init__(self, src, dst, send, recv, slot, target):
        self.copies = [
            pltpu.make_async_remote_copy(
                src_ref=piece,
                dst_ref=landing,
                send_sem=send.at[slot + (k,)],
                recv_sem=recv.at[slot + (k,)],
                device_id=target,
                device_id_type=MESH,
            )
            for k, (piece, landing) in enumerate(zip(src, dst))
        ]

    def start(self):
        for copy in self.copies:
            copy.start()

    def wait_recv(self):
        for copy in self.copies:
            copy.wait_recv()

    def wait_send(self):
        for copy in self.copies:
            copy.wait_send()


def at(refs, *index):
    return [ref.at[index] for ref in refs]


def dispatch_kernel(experts, groups, pieces, *refs):
    bucket, out = refs[:pieces], refs[pieces : 2 * pieces]
    own_sem, a_send, a_recv, b_send, b_recv, c_send, c_recv = refs[2 * pieces :]
    mine, block, near, far, corner, device = place(groups)
    greet(mine, block, near, far, device, experts)

    order = rounds(experts, groups)
    spread, to_near, to_far, relay = {}, {}, {}, {}
    for r in reversed(order[1:]):
        peer = (mine + r) % experts
        spread[r] = Transfer(at(bucket, peer), at(out, block, mine), a_send, a_recv, (r,), device(peer, block))
        spread[r].start()
    own = [
        pltpu.make_async_copy(src, dst, own_sem.at[k])
        for k, (src, dst) in enumerate(zip(at(bucket, mine), at(out, block, mine)))
    ]
    for copy in own:
        copy.start()

    def forward(r):
        source = (mine + experts - r) % experts
        if over_far(r):
            to_near[r].wait_recv()
            moved = at(out, near, source)
            relay[r] = Transfer(moved, moved, c_send, c_recv, (r,), device(mine, far))
        else:
            to_far[r].wait_recv()
            moved = at(out, far, source)
            relay[r] = Transfer(moved, moved, c_send, c_recv, (r,), device(mine, near))
        relay[r].start()

    for step, r in enumerate(order):
        source = (mine + experts - r) % experts
        dst = at(out, block, source)
        if r == 0:
            src = at(bucket, mine)
        else:
            spread[r].wait_recv()
            src = dst
        to_near[r] = Transfer(src, dst, b_send, b_recv, (0, r), device(mine, near))
        to_far[r] = Transfer(src, dst, b_send, b_recv, (1, r), device(mine, far))
        to_near[r].start()
        to_far[r].start()
        if step >= LAG:
            forward(order[step - LAG])
    for r in order[experts - LAG :]:
        forward(r)
    for r in order:
        if over_far(r):
            to_far[r].wait_recv()
        else:
            to_near[r].wait_recv()
        relay[r].wait_recv()
    for r in order:
        if r:
            spread[r].wait_send()
        to_near[r].wait_send()
        to_far[r].wait_send()
        relay[r].wait_send()
    for copy in own:
        copy.wait()


def combine_kernel(experts, groups, pieces, *refs):
    part, ret, held, total, back = [refs[k * pieces : (k + 1) * pieces] for k in range(5)]
    a_send, a_recv, b_send, b_recv, c_send, c_recv = refs[5 * pieces :]
    mine, block, near, far, corner, device = place(groups)
    greet(mine, block, near, far, device, experts)

    def add(dst, *terms):
        for k in range(pieces):
            value = terms[0][k][...].astype(jnp.float32)
            for term in terms[1:]:
                value = value + term[k][...].astype(jnp.float32)
            dst[k][...] = value.astype(dst[k].dtype)

    order = rounds(experts, groups)[::-1]
    relay, to_near, to_far, home = {}, {}, {}, {}

    def open_round(r):
        source = (mine + experts - r) % experts
        target = far if over_far(r) else near
        relay[r] = Transfer(at(part, corner, source), at(held, 2, r), c_send, c_recv, (r,), device(mine, target))
        relay[r].start()
        if over_far(r):
            to_far[r] = Transfer(at(part, far, source), at(held, 1, r), b_send, b_recv, (1, r), device(mine, far))
            to_far[r].start()
        else:
            to_near[r] = Transfer(at(part, near, source), at(held, 0, r), b_send, b_recv, (0, r), device(mine, near))
            to_near[r].start()

    def send_home(r):
        source = (mine + experts - r) % experts
        to_near[r].wait_recv()
        to_far[r].wait_recv()
        terms = at(part, block, source), at(held, 0, r), at(held, 1, r)
        if r == 0:
            add(at(ret, mine), *terms)
        else:
            add(at(back, r), *terms)
            home[r] = Transfer(at(back, r), at(ret, mine), a_send, a_recv, (r,), device(source, block))
            home[r].start()

    for r in order[:AHEAD]:
        open_round(r)
    for step, r in enumerate(order):
        source = (mine + experts - r) % experts
        relay[r].wait_recv()
        if over_far(r):
            add(at(total, r), at(part, near, source), at(held, 2, r))
            to_near[r] = Transfer(at(total, r), at(held, 0, r), b_send, b_recv, (0, r), device(mine, near))
            to_near[r].start()
        else:
            add(at(total, r), at(part, far, source), at(held, 2, r))
            to_far[r] = Transfer(at(total, r), at(held, 1, r), b_send, b_recv, (1, r), device(mine, far))
            to_far[r].start()
        if step + AHEAD < experts:
            open_round(order[step + AHEAD])
        if step >= LAG:
            send_home(order[step - LAG])
    for r in order[experts - LAG :]:
        send_home(r)
    for r in order:
        if r:
            home[r].wait_recv()
            home[r].wait_send()
        relay[r].wait_send()
        to_near[r].wait_send()
        to_far[r].wait_send()


def sems(experts, pieces):
    dma = pltpu.SemaphoreType.DMA
    one, two = dma((experts, pieces)), dma((2, experts, pieces))
    return [one, one, two, two, one, one]


def dispatch(bucket, groups):
    experts, pieces = bucket[0].shape[0], len(bucket)
    return pl.pallas_call(
        functools.partial(dispatch_kernel, experts, groups, pieces),
        out_shape=[jax.ShapeDtypeStruct((SHARDS,) + piece.shape, piece.dtype) for piece in bucket],
        in_specs=[pl.BlockSpec(memory_space=pltpu.VMEM)] * pieces,
        out_specs=[pl.BlockSpec(memory_space=pl.ANY)] * pieces,
        scratch_shapes=[pltpu.SemaphoreType.DMA((pieces,))] + sems(experts, pieces),
        compiler_params=pltpu.CompilerParams(collective_id=0, has_side_effects=True),
        name="dispatch",
    )(*bucket)


def combine(part, groups):
    experts, pieces = part[0].shape[1], len(part)
    blocks = [(piece.shape[1:], piece.dtype) for piece in part]
    return pl.pallas_call(
        functools.partial(combine_kernel, experts, groups, pieces),
        out_shape=[jax.ShapeDtypeStruct(shape, kind) for shape, kind in blocks],
        in_specs=[pl.BlockSpec(memory_space=pltpu.VMEM)] * pieces,
        out_specs=[pl.BlockSpec(memory_space=pltpu.VMEM)] * pieces,
        scratch_shapes=[pltpu.VMEM((3,) + shape, kind) for shape, kind in blocks]
        + [pltpu.VMEM(shape, kind) for shape, kind in blocks] * 2
        + sems(experts, pieces),
        compiler_params=pltpu.CompilerParams(
            collective_id=1, has_side_effects=True, vmem_limit_bytes=60 * 2**20
        ),
        name="combine",
    )(*part)


def dot(left, right):
    return jnp.dot(left, right, preferred_element_type=jnp.float32)


def activate(gate_act, up_act):
    return (jax.nn.silu(gate_act) * up_act).astype(jnp.bfloat16)


def expert_block(rows, w_gate, w_up, w_down):
    hidden = activate(dot(rows, w_gate), dot(rows, w_up))
    return dot(hidden, w_down).astype(jnp.bfloat16)


def folded_block(rows, w_gate, w_up, w_down):
    half = rows.shape[1]

    def project(weight):
        left = dot(rows, weight[:half]).reshape(-1, 2, FOLD, weight.shape[1])
        right = dot(rows, weight[half:]).reshape(-1, 2, FOLD, weight.shape[1])
        return left[:, 0] + right[:, 1]

    hidden = activate(project(w_gate), project(w_up))
    twice = jnp.concatenate([hidden, hidden], axis=1).reshape(rows.shape[0], -1)
    upper = jnp.arange(rows.shape[0])[:, None] % (2 * FOLD) < FOLD
    return jnp.where(upper, dot(twice, w_down[:, :half]), dot(twice, w_down[:, half:])).astype(jnp.bfloat16)


def per_device(tokens, routes, scores, gate_proj, up_proj, down_proj):
    node_count = lax.axis_size("node")
    local_count = lax.axis_size("local")
    token_count, model_width = tokens.shape
    top_count = routes.shape[1]
    groups = local_count // SHARDS
    experts = node_count * groups
    per_expert = max(
        2, token_count * top_count // experts + token_count * top_count // (4 * experts)
    )
    tile = 2 * FOLD
    half = model_width // 2
    full = per_expert // tile * tile
    folds = full > 0 and 0 < per_expert - full <= FOLD
    if not folds:
        full = (per_expert + tile - 1) // tile * tile
    cap = full + FOLD if folds else full
    weights = (SCALE * scores / jnp.sum(scores, axis=1, keepdims=True)).astype(jnp.bfloat16)
    labels = jnp.arange(experts, dtype=jnp.int32)
    matches = routes[:, :, None] == labels[None, None, :]
    routed = jnp.any(matches, axis=1)
    dense_weight = jnp.sum(jnp.where(matches, weights.astype(jnp.float32)[:, :, None], 0.0), axis=1)
    position = jnp.cumsum(routed.astype(jnp.int32), axis=0) - 1
    slot_ids = jnp.arange(cap, dtype=jnp.int32)
    pick = routed.T[:, None, :] & (position.T[:, None, :] == slot_ids[None, :, None])
    slot_pick = pick.astype(jnp.bfloat16)
    slot_weight = jnp.where(pick, dense_weight.T[:, None, :], 0.0).astype(jnp.bfloat16)

    def flat(slots):
        return slots.reshape(-1, slots.shape[-1])

    def halves(slots):
        none = jnp.zeros_like(slots)
        return flat(jnp.concatenate([slots, none], axis=1)), flat(jnp.concatenate([none, slots], axis=1))

    bucket = [dot(flat(slot_pick[:, :full]), tokens).astype(jnp.bfloat16).reshape(experts, full, model_width)]
    if folds:
        upper, lower = halves(slot_pick[:, full:])
        folded = (dot(upper, tokens[:, :half]) + dot(lower, tokens[:, half:])).astype(jnp.bfloat16)
        bucket.append(folded.reshape(experts, tile, half))
    gathered = dispatch(bucket, groups)
    blocks = expert_block, folded_block
    part = [
        blocks[k](flat(piece), gate_proj[0], up_proj[0], down_proj[0]).reshape(piece.shape)
        for k, piece in enumerate(gathered)
    ]
    returned = combine(part, groups)
    combined = dot(flat(slot_weight[:, :full]).T, flat(returned[0]))
    if folds:
        upper, lower = halves(slot_weight[:, full:])
        rows = flat(returned[1])
        combined = combined + jnp.concatenate([dot(upper.T, rows), dot(lower.T, rows)], axis=1)
    return combined.astype(jnp.bfloat16)


def solution(mesh):
    return jax.shard_map(
        per_device,
        mesh=mesh,
        in_specs=(
            P(("node", "local"), None),
            P(("node", "local"), None),
            P(("node", "local"), None),
            P(("node", "local"), None, None),
            P(("node", "local"), None, None),
            P(("node", "local"), None, None),
        ),
        out_specs=P(("node", "local"), None),
        check_vma=False,
    )
```

```python
import functools

import jax
import jax.numpy as jnp
from jax import lax
from jax.experimental import pallas as pl
from jax.experimental.pallas import tpu as pltpu
from jax.sharding import PartitionSpec as P

SHARDS = 4
SCALE = 2.827
FOLD = 4
MESH = pl.DeviceIdType.MESH


def place(groups):
    node = lax.axis_index("node")
    local = lax.axis_index("local")
    mine = node * groups + local // SHARDS
    block = local % SHARDS
    near = block + 1 - 2 * (block % 2)
    far = (block + 2) % SHARDS
    corner = (near + 2) % SHARDS

    def device(expert, which):
        return (expert // groups, (expert % groups) * SHARDS + which)

    return mine, block, near, far, corner, device


def greet(mine, block, near, far, device, experts):
    barrier = pltpu.get_barrier_semaphore()
    targets = [device((mine + r) % experts, block) for r in range(1, experts)]
    targets += [device(mine, near), device(mine, far)]
    for target in targets:
        pl.semaphore_signal(barrier, inc=1, device_id=target, device_id_type=MESH)
    pl.semaphore_wait(barrier, len(targets))


def over_far(r, every):
    return every > 0 and r % every == 0


def rounds(experts, groups):
    same = [r for r in range(experts) if r % groups == 0]
    return same + [r for r in range(experts) if r % groups]


DISPATCH_FAR = 4
COMBINE_FAR = 0
AHEAD = 4
LAG = 2


class Transfer:
    def __init__(self, src, dst, send, recv, slot, target):
        self.copies = [
            pltpu.make_async_remote_copy(
                src_ref=piece,
                dst_ref=landing,
                send_sem=send.at[slot + (k,)],
                recv_sem=recv.at[slot + (k,)],
                device_id=target,
                device_id_type=MESH,
            )
            for k, (piece, landing) in enumerate(zip(src, dst))
        ]

    def start(self):
        for copy in self.copies:
            copy.start()

    def wait_recv(self):
        for copy in self.copies:
            copy.wait_recv()

    def wait_send(self):
        for copy in self.copies:
            copy.wait_send()


def at(refs, *index):
    return [ref.at[index] for ref in refs]


def dispatch_kernel(experts, groups, pieces, *refs):
    bucket, out = refs[:pieces], refs[pieces : 2 * pieces]
    own_sem, a_send, a_recv, b_send, b_recv, c_send, c_recv = refs[2 * pieces :]
    mine, block, near, far, corner, device = place(groups)
    greet(mine, block, near, far, device, experts)

    order = rounds(experts, groups)
    spread, to_near, to_far, relay = {}, {}, {}, {}
    for r in reversed(order[1:]):
        peer = (mine + r) % experts
        spread[r] = Transfer(at(bucket, peer), at(out, block, mine), a_send, a_recv, (r,), device(peer, block))
        spread[r].start()
    own = [
        pltpu.make_async_copy(src, dst, own_sem.at[k])
        for k, (src, dst) in enumerate(zip(at(bucket, mine), at(out, block, mine)))
    ]
    for copy in own:
        copy.start()

    def forward(r):
        source = (mine + experts - r) % experts
        if over_far(r, DISPATCH_FAR):
            to_near[r].wait_recv()
            moved = at(out, near, source)
            relay[r] = Transfer(moved, moved, c_send, c_recv, (r,), device(mine, far))
        else:
            to_far[r].wait_recv()
            moved = at(out, far, source)
            relay[r] = Transfer(moved, moved, c_send, c_recv, (r,), device(mine, near))
        relay[r].start()

    for step, r in enumerate(order):
        source = (mine + experts - r) % experts
        dst = at(out, block, source)
        if r == 0:
            src = at(bucket, mine)
        else:
            spread[r].wait_recv()
            src = dst
        to_near[r] = Transfer(src, dst, b_send, b_recv, (0, r), device(mine, near))
        to_far[r] = Transfer(src, dst, b_send, b_recv, (1, r), device(mine, far))
        to_near[r].start()
        to_far[r].start()
        if step >= LAG:
            forward(order[step - LAG])
    for r in order[experts - LAG :]:
        forward(r)
    for r in order:
        if over_far(r, DISPATCH_FAR):
            to_far[r].wait_recv()
        else:
            to_near[r].wait_recv()
        relay[r].wait_recv()
    for r in order:
        if r:
            spread[r].wait_send()
        to_near[r].wait_send()
        to_far[r].wait_send()
        relay[r].wait_send()
    for copy in own:
        copy.wait()


def combine_kernel(experts, groups, pieces, *refs):
    part, ret, held, total, back = [refs[k * pieces : (k + 1) * pieces] for k in range(5)]
    a_send, a_recv, b_send, b_recv, c_send, c_recv = refs[5 * pieces :]
    mine, block, near, far, corner, device = place(groups)
    greet(mine, block, near, far, device, experts)

    def add(dst, *terms):
        for k in range(pieces):
            value = terms[0][k][...].astype(jnp.float32)
            for term in terms[1:]:
                value = value + term[k][...].astype(jnp.float32)
            dst[k][...] = value.astype(dst[k].dtype)

    order = rounds(experts, groups)[::-1]
    relay, to_near, to_far, home = {}, {}, {}, {}

    def open_round(r):
        source = (mine + experts - r) % experts
        target = far if over_far(r, COMBINE_FAR) else near
        relay[r] = Transfer(at(part, corner, source), at(held, 2, r), c_send, c_recv, (r,), device(mine, target))
        relay[r].start()
        if over_far(r, COMBINE_FAR):
            to_far[r] = Transfer(at(part, far, source), at(held, 1, r), b_send, b_recv, (1, r), device(mine, far))
            to_far[r].start()
        else:
            to_near[r] = Transfer(at(part, near, source), at(held, 0, r), b_send, b_recv, (0, r), device(mine, near))
            to_near[r].start()

    def send_home(r):
        source = (mine + experts - r) % experts
        to_near[r].wait_recv()
        to_far[r].wait_recv()
        terms = at(part, block, source), at(held, 0, r), at(held, 1, r)
        if r == 0:
            add(at(ret, mine), *terms)
        else:
            add(at(back, r), *terms)
            home[r] = Transfer(at(back, r), at(ret, mine), a_send, a_recv, (r,), device(source, block))
            home[r].start()

    for r in order[:AHEAD]:
        open_round(r)
    for step, r in enumerate(order):
        source = (mine + experts - r) % experts
        relay[r].wait_recv()
        if over_far(r, COMBINE_FAR):
            add(at(total, r), at(part, near, source), at(held, 2, r))
            to_near[r] = Transfer(at(total, r), at(held, 0, r), b_send, b_recv, (0, r), device(mine, near))
            to_near[r].start()
        else:
            add(at(total, r), at(part, far, source), at(held, 2, r))
            to_far[r] = Transfer(at(total, r), at(held, 1, r), b_send, b_recv, (1, r), device(mine, far))
            to_far[r].start()
        if step + AHEAD < experts:
            open_round(order[step + AHEAD])
        if step >= LAG:
            send_home(order[step - LAG])
    for r in order[experts - LAG :]:
        send_home(r)
    for r in order:
        if r:
            home[r].wait_recv()
            home[r].wait_send()
        relay[r].wait_send()
        to_near[r].wait_send()
        to_far[r].wait_send()


def sems(experts, pieces):
    dma = pltpu.SemaphoreType.DMA
    one, two = dma((experts, pieces)), dma((2, experts, pieces))
    return [one, one, two, two, one, one]


def dispatch(bucket, groups):
    experts, pieces = bucket[0].shape[0], len(bucket)
    return pl.pallas_call(
        functools.partial(dispatch_kernel, experts, groups, pieces),
        out_shape=[jax.ShapeDtypeStruct((SHARDS,) + piece.shape, piece.dtype) for piece in bucket],
        in_specs=[pl.BlockSpec(memory_space=pltpu.VMEM)] * pieces,
        out_specs=[pl.BlockSpec(memory_space=pl.ANY)] * pieces,
        scratch_shapes=[pltpu.SemaphoreType.DMA((pieces,))] + sems(experts, pieces),
        compiler_params=pltpu.CompilerParams(collective_id=0, has_side_effects=True),
        name="dispatch",
    )(*bucket)


def combine(part, groups):
    experts, pieces = part[0].shape[1], len(part)
    blocks = [(piece.shape[1:], piece.dtype) for piece in part]
    return pl.pallas_call(
        functools.partial(combine_kernel, experts, groups, pieces),
        out_shape=[jax.ShapeDtypeStruct(shape, kind) for shape, kind in blocks],
        in_specs=[pl.BlockSpec(memory_space=pltpu.VMEM)] * pieces,
        out_specs=[pl.BlockSpec(memory_space=pltpu.VMEM)] * pieces,
        scratch_shapes=[pltpu.VMEM((3,) + shape, kind) for shape, kind in blocks]
        + [pltpu.VMEM(shape, kind) for shape, kind in blocks] * 2
        + sems(experts, pieces),
        compiler_params=pltpu.CompilerParams(
            collective_id=1, has_side_effects=True, vmem_limit_bytes=60 * 2**20
        ),
        name="combine",
    )(*part)


def dot(left, right):
    return jnp.dot(left, right, preferred_element_type=jnp.float32)


def activate(gate_act, up_act):
    return (jax.nn.silu(gate_act) * up_act).astype(jnp.bfloat16)


def expert_block(rows, w_gate, w_up, w_down):
    hidden = activate(dot(rows, w_gate), dot(rows, w_up))
    return dot(hidden, w_down).astype(jnp.bfloat16)


def folded_block(rows, w_gate, w_up, w_down):
    half = rows.shape[1]

    def project(weight):
        left = dot(rows, weight[:half]).reshape(-1, 2, FOLD, weight.shape[1])
        right = dot(rows, weight[half:]).reshape(-1, 2, FOLD, weight.shape[1])
        return left[:, 0] + right[:, 1]

    hidden = activate(project(w_gate), project(w_up))
    twice = jnp.concatenate([hidden, hidden], axis=1).reshape(rows.shape[0], -1)
    upper = jnp.arange(rows.shape[0])[:, None] % (2 * FOLD) < FOLD
    return jnp.where(upper, dot(twice, w_down[:, :half]), dot(twice, w_down[:, half:])).astype(jnp.bfloat16)


def per_device(tokens, routes, scores, gate_proj, up_proj, down_proj):
    node_count = lax.axis_size("node")
    local_count = lax.axis_size("local")
    token_count, model_width = tokens.shape
    top_count = routes.shape[1]
    groups = local_count // SHARDS
    experts = node_count * groups
    per_expert = max(
        2, token_count * top_count // experts + token_count * top_count // (4 * experts)
    )
    tile = 2 * FOLD
    half = model_width // 2
    full = per_expert // tile * tile
    folds = full > 0 and 0 < per_expert - full <= FOLD
    if not folds:
        full = (per_expert + tile - 1) // tile * tile
    cap = full + FOLD if folds else full
    weights = (SCALE * scores / jnp.sum(scores, axis=1, keepdims=True)).astype(jnp.bfloat16)
    labels = jnp.arange(experts, dtype=jnp.int32)
    matches = routes[:, :, None] == labels[None, None, :]
    routed = jnp.any(matches, axis=1)
    dense_weight = jnp.sum(jnp.where(matches, weights.astype(jnp.float32)[:, :, None], 0.0), axis=1)
    position = jnp.cumsum(routed.astype(jnp.int32), axis=0) - 1
    slot_ids = jnp.arange(cap, dtype=jnp.int32)
    pick = routed.T[:, None, :] & (position.T[:, None, :] == slot_ids[None, :, None])
    slot_pick = pick.astype(jnp.bfloat16)
    slot_weight = jnp.where(pick, dense_weight.T[:, None, :], 0.0).astype(jnp.bfloat16)

    def flat(slots):
        return slots.reshape(-1, slots.shape[-1])

    def halves(slots):
        none = jnp.zeros_like(slots)
        return flat(jnp.concatenate([slots, none], axis=1)), flat(jnp.concatenate([none, slots], axis=1))

    bucket = [dot(flat(slot_pick[:, :full]), tokens).astype(jnp.bfloat16).reshape(experts, full, model_width)]
    if folds:
        upper, lower = halves(slot_pick[:, full:])
        folded = (dot(upper, tokens[:, :half]) + dot(lower, tokens[:, half:])).astype(jnp.bfloat16)
        bucket.append(folded.reshape(experts, tile, half))
    gathered = dispatch(bucket, groups)
    blocks = expert_block, folded_block
    part = [
        blocks[k](flat(piece), gate_proj[0], up_proj[0], down_proj[0]).reshape(piece.shape)
        for k, piece in enumerate(gathered)
    ]
    returned = combine(part, groups)
    combined = dot(flat(slot_weight[:, :full]).T, flat(returned[0]))
    if folds:
        upper, lower = halves(slot_weight[:, full:])
        rows = flat(returned[1])
        combined = combined + jnp.concatenate([dot(upper.T, rows), dot(lower.T, rows)], axis=1)
    return combined.astype(jnp.bfloat16)


def solution(mesh):
    return jax.shard_map(
        per_device,
        mesh=mesh,
        in_specs=(
            P(("node", "local"), None),
            P(("node", "local"), None),
            P(("node", "local"), None),
            P(("node", "local"), None, None),
            P(("node", "local"), None, None),
            P(("node", "local"), None, None),
        ),
        out_specs=P(("node", "local"), None),
        check_vma=False,
    )
```
